256 devices in a mesh: lat: 32 (over y_hi, z, core), lon: 8 (over y_lo, x).
Axes of the slice: x: 4, y: 4 (y_hi: 2, y_lo: 2; y = y_hi * 2 + y_lo), z: 8, core: 2. Of those that a mesh axis runs over, the one named last changes fastest.
Arguments:
- features: bfloat16 [512, 512, 512], P('lat', 'lon'), may hold values from -6 to 6
- upstream: bfloat16 [512, 512, 512], P('lat', 'lon'), may hold values from -6 to 6
- kernel: bfloat16 [4608, 512], replicated, may hold values from -0.09375 to 0.09375
Outputs:
- input_grad: bfloat16 [512, 512, 512], P('lat', 'lon')
- direction: float32 [4608, 512], P('lat')
- perturbed: float32 [4608, 512], P('lat')
The draws below stay inside these ranges and needn't reach their ends.
All inputs are finite; a program needn't handle non-finite values.
Results may differ from the reference program's by a relative error of at most 0.0032.
Values may be sent and summed in bfloat16 or wider, within the bound.
No kernel may reach another device: no remote copies, remote signals or barrier semaphores. Data moves between devices by JAX's collectives and lax.ppermute only.
A program may use at most 128 MiB of HBM per device.

```python
import jax
import jax.numpy as jnp
from jax import lax

C = 512
NLAT = 512
NLON = 512


def block_levels(stream_key, extent, pieces, low, top_value):
    level, own = 1.0, jax.random.fold_in(stream_key, 6)
    for dim, blocks in pieces:
        draws = jnp.exp(jax.random.uniform(jax.random.fold_in(own, dim), (blocks,), jnp.float32, low / len(pieces), top_value / len(pieces)))
        level = level * jnp.repeat(draws, extent[dim] // blocks).reshape([-1 if axis == dim else 1 for axis in range(len(extent))])
    return level


def centred(key, dims, spread, most, split=(), held_as=jnp.bfloat16):
    entries = spread * jax.random.normal(key, dims, jnp.float32)
    if split:
        entries = entries * block_levels(key, dims, split, -0.22, 0.18)
    return jnp.clip(entries, -most, most).astype(held_as)


def setup_inputs(seed: int = 0) -> dict:
    arg_keys = jax.random.split(jax.random.key(seed), 4)
    return {
        "features": centred(arg_keys[0], (NLAT, NLON, C), 1.0, 6.0, ((0, 32), (1, 8))),
        "upstream": centred(arg_keys[1], (NLAT, NLON, C), 1.0, 6.0, ((0, 32), (1, 8))),
        "kernel": centred(arg_keys[2], (9 * C, C), (9 * C) ** -0.5, 0.09375),
    }


def extend(field):
    wrapped = jnp.concatenate([field[:, -1:], field, field[:, :1]], axis=1)
    return jnp.pad(wrapped, ((1, 1), (0, 0), (0, 0)))

def reference(features, upstream, kernel):
    height, breadth, channels = features.shape
    padded_x = extend(features)
    z = jnp.zeros((height, breadth, channels), jnp.float32)
    for a in range(3):
        for b in range(3):
            t = 3 * a + b
            z = z + jnp.dot(padded_x[a:a + height, b:b + breadth], kernel[t * channels:(t + 1) * channels], preferred_element_type=jnp.float32)
    sig = jax.nn.sigmoid(z)
    slope = (upstream.astype(jnp.float32) * sig * (1.0 + z * (1.0 - sig))).astype(jnp.bfloat16)
    padded_slope = extend(slope)
    back = upstream.astype(jnp.float32)
    blocks = []
    for a in range(3):
        for b in range(3):
            t = 3 * a + b
            piece = padded_slope[2 - a:2 - a + height, 2 - b:2 - b + breadth]
            back = back + lax.dot_general(piece, kernel[t * channels:(t + 1) * channels], (((2,), (1,)), ((), ())), preferred_element_type=jnp.float32)
            blocks.append(lax.dot_general(padded_x[a:a + height, b:b + breadth], slope, (((0, 1), (0, 1)), ((), ())), preferred_element_type=jnp.float32))
    input_grad = back.astype(jnp.bfloat16)
    grad = jnp.concatenate(blocks, axis=0)
    count = 9.0 * channels * channels
    total = jnp.sum(grad * grad)
    direction = grad / jnp.sqrt(total / count + 1e-06)
    perturbed = kernel.astype(jnp.float32) + 0.05 / jnp.sqrt(count) * direction
    return (input_grad, direction, perturbed)
```

```python
import jax
import jax.numpy as jnp
from jax import lax
from jax.sharding import Mesh, PartitionSpec as P

SPLIT = (("yh", 2), ("z", 8), ("core", 2), ("yl", 2), ("x", 4))
LAT = ("yh", "z", "core")
LON = ("yl", "x")
Y = ("yh", "yl")


def ring(count, step):
    return [(i, (i + step) % count) for i in range(count)]


def padded_2(block, sides, width, periodic):
    for axis, dim in sides:
        count = lax.axis_size(axis)
        forward = [(i, i + 1) for i in range(count - 1)]
        if periodic:
            forward.append((count - 1, 0))
        backward = [(target, source) for source, target in forward]
        low = lax.ppermute(
            lax.slice_in_dim(block, block.shape[dim] - width, None, axis=dim), axis, forward
        )
        high = lax.ppermute(lax.slice_in_dim(block, 0, width, axis=dim), axis, backward)
        block = jnp.concatenate([low, block, high], axis=dim)
    return block


def padded(field):
    return padded_2(padded_2(field, ((LON, 1),), 1, True), ((LAT, 0),), 1, False)


def convolve(padded, kernel, height, breadth):
    channels = kernel.shape[1]
    total = jnp.zeros((height, breadth, channels), jnp.float32)
    for a in range(3):
        for b in range(3):
            t = 3 * a + b
            total = total + jnp.dot(
                padded[a : a + height, b : b + breadth],
                kernel[t * channels : (t + 1) * channels],
                preferred_element_type=jnp.float32,
            )
    return total


def spread(padded, kernel, height, breadth):
    channels = kernel.shape[1]
    total = jnp.zeros((height, breadth, channels), jnp.float32)
    for a in range(3):
        for b in range(3):
            t = 3 * a + b
            piece = padded[2 - a : 2 - a + height, 2 - b : 2 - b + breadth]
            total = total + lax.dot_general(
                piece,
                kernel[t * channels : (t + 1) * channels],
                (((2,), (1,)), ((), ())),
                preferred_element_type=jnp.float32,
            )
    return total


def weight_terms(padded, slope, height, breadth):
    blocks = []
    for a in range(3):
        for b in range(3):
            blocks.append(
                lax.dot_general(
                    padded[a : a + height, b : b + breadth],
                    slope,
                    (((0, 1), (0, 1)), ((), ())),
                    preferred_element_type=jnp.float32,
                )
            )
    return jnp.concatenate(blocks, axis=0)


def gated(upstream, z):
    sig = jax.nn.sigmoid(z)
    return upstream.astype(jnp.float32) * sig * (1.0 + z * (1.0 - sig))


def take(pieces, index):
    return lax.dynamic_index_in_dim(pieces, index, 0, keepdims=False)


def scattered(pieces, axis, count):
    me = lax.axis_index(axis)
    came = []
    for step in (1, 3, 2):
        goes = take(pieces, (me + step) % count).astype(jnp.bfloat16)
        came.append(lax.ppermute(goes, axis, ring(count, step)))
    total = take(pieces, me)
    for piece in came:
        total = total + piece.astype(jnp.float32)
    return total


def shards(features, upstream, kernel):
    height, breadth, channels = features.shape
    padded_x = padded(features)
    z = convolve(padded_x, kernel, height, breadth)
    slope = gated(upstream, z).astype(jnp.bfloat16)

    local_grad = weight_terms(padded_x, slope, height, breadth)
    by_core = local_grad.reshape(16, 2, 144, channels)
    core = lax.axis_index("core")
    goes = lax.dynamic_index_in_dim(by_core, 1 - core, 1, keepdims=False).astype(jnp.bfloat16)
    came = lax.ppermute(goes, "core", [(0, 1), (1, 0)])
    mine = lax.dynamic_index_in_dim(by_core, core, 1, keepdims=False) + came.astype(jnp.float32)
    parts = mine.reshape(2, 2, 4, 2, 72, 4, 128)
    low = jnp.moveaxis(parts[:, 0], 4, 0)
    high = parts[:, 1].transpose(0, 2, 1, 3, 4, 5).reshape(4, 4, 72, 4, 128)
    low = scattered(low, "x", 4)
    high = scattered(high, Y, 4)
    low = low.transpose(0, 2, 1, 3, 4).reshape(4, 4, 72, 128)
    high = high.transpose(2, 0, 1, 3)
    low = scattered(low, Y, 4)
    high = scattered(high, "x", 4)
    plane = jnp.concatenate([low, high], axis=0)
    chunk = lax.all_to_all(plane, "z", 0, 0, tiled=True).sum(axis=0)
    everyone = lax.all_to_all(jnp.broadcast_to(chunk[None], (8, 72, 128)), LON, 0, 0, tiled=True)
    summed = everyone.reshape(2, 4, 72, 128).transpose(0, 2, 1, 3).reshape(144, channels)
    part = jnp.sum(everyone * everyone)
    total = lax.all_to_all(jnp.broadcast_to(part[None], (32,)), LAT, 0, 0, tiled=True).sum()

    padded_slope = padded(slope)
    back = upstream.astype(jnp.float32) + spread(padded_slope, kernel, height, breadth)
    input_grad = back.astype(jnp.bfloat16)

    count = 9.0 * channels * channels
    direction = summed / jnp.sqrt(total / count + 1e-06)
    block_rows = summed.shape[0]
    start = lax.axis_index(LAT) * block_rows
    own_kernel = lax.dynamic_slice_in_dim(kernel, start, block_rows, 0)
    perturbed = own_kernel.astype(jnp.float32) + 0.05 / jnp.sqrt(count) * direction
    return (input_grad, direction, perturbed)


def solution(mesh):
    names, sizes = zip(*SPLIT)
    fine = Mesh(mesh.devices.reshape(sizes), names)
    return jax.shard_map(
        shards,
        mesh=fine,
        in_specs=(P(LAT, LON, None), P(LAT, LON, None), P()),
        out_specs=(P(LAT, LON, None), P(LAT, None), P(LAT, None)),
        check_vma=False,
    )
```

```python
import jax
import jax.numpy as jnp
from jax import lax
from jax.experimental import pallas as pl
from jax.experimental.pallas import tpu as pltpu
from jax.sharding import Mesh, PartitionSpec as P

SPLIT = (("yh", 2), ("z", 8), ("core", 2), ("yl", 2), ("x", 4))
LAT = ("yh", "z", "core")
LON = ("yl", "x")
Y = ("yh", "yl")


def ring(count, step):
    return [(i, (i + step) % count) for i in range(count)]


def padded_2(block, sides, width, periodic):
    for axis, dim in sides:
        count = lax.axis_size(axis)
        forward = [(i, i + 1) for i in range(count - 1)]
        if periodic:
            forward.append((count - 1, 0))
        backward = [(target, source) for source, target in forward]
        low = lax.ppermute(
            lax.slice_in_dim(block, block.shape[dim] - width, None, axis=dim), axis, forward
        )
        high = lax.ppermute(lax.slice_in_dim(block, 0, width, axis=dim), axis, backward)
        block = jnp.concatenate([low, block, high], axis=dim)
    return block


def padded(field):
    return padded_2(padded_2(field, ((LON, 1),), 1, True), ((LAT, 0),), 1, False)


def lay_out(padded_ref, wide_ref):
    def row(r, carry):
        for b in range(3):
            wide_ref[pl.ds(pl.multiple_of(64 * r, 64), 64), 512 * b : 512 * (b + 1)] = padded_ref[r, b : b + 64, :]
        return carry

    lax.fori_loop(0, 18, row, 0)


def forward_kernel(padded_ref, kernel_ref, upstream_ref, slope_ref, goes_ref, mine_ref, wide_ref, grad_ref):
    lay_out(padded_ref, wide_ref)

    def cells(m, carry):
        z = None
        for a in range(3):
            rows = pl.ds(pl.multiple_of(256 * m + 64 * a, 64), 256)
            term = jnp.dot(
                wide_ref[rows, :], kernel_ref[1536 * a : 1536 * (a + 1), :], preferred_element_type=jnp.float32
            )
            z = term if z is None else z + term
        sig = jax.nn.sigmoid(z)
        here = pl.ds(pl.multiple_of(256 * m, 256), 256)
        gate = upstream_ref[here, :].astype(jnp.float32) * sig * (1.0 + z * (1.0 - sig))
        slope_ref[here, :] = gate.astype(jnp.bfloat16)
        return carry

    lax.fori_loop(0, 4, cells, 0)
    for a in range(3):

        def tap(b, carry):
            taken = wide_ref[64 * a : 64 * a + 1024, pl.ds(pl.multiple_of(512 * b, 512), 512)]
            term = lax.dot_general(
                taken, slope_ref[...], (((0,), (0,)), ((), ())), preferred_element_type=jnp.float32
            )
            grad_ref[pl.ds(pl.multiple_of(1536 * a + 512 * b, 512), 512), :] = term
            return carry

        lax.fori_loop(0, 3, tap, 0)
    core = lax.axis_index("core")

    def part(k, carry):
        away = pl.multiple_of(144 * (2 * k + 1 - core), 144)
        goes_ref[k] = grad_ref[pl.ds(away, 144), :].astype(jnp.bfloat16)
        kept = pl.multiple_of(144 * (2 * k + core), 144)
        mine_ref[k] = grad_ref[pl.ds(kept, 144), :]
        return carry

    lax.fori_loop(0, 16, part, 0)


def spread_kernel(padded_ref, kernel_ref, upstream_ref, out_ref, wide_ref):
    lay_out(padded_ref, wide_ref)

    def cells(m, carry):
        here = pl.ds(pl.multiple_of(256 * m, 256), 256)
        total = upstream_ref[here, :].astype(jnp.float32)
        for a in range(3):
            rows = pl.ds(pl.multiple_of(256 * m + 64 * (2 - a), 64), 256)
            for b in range(3):
                t = 3 * a + b
                total = total + lax.dot_general(
                    wide_ref[rows, 512 * (2 - b) : 512 * (3 - b)],
                    kernel_ref[512 * t : 512 * (t + 1), :],
                    (((1,), (1,)), ((), ())),
                    preferred_element_type=jnp.float32,
                )
        out_ref[here, :] = total.astype(jnp.bfloat16)
        return carry

    lax.fori_loop(0, 4, cells, 0)


VMEM = pl.BlockSpec(memory_space=pltpu.VMEM)
FLOPS = 2 * 1024 * 4608 * 512


def forward(padded_x, kernel, upstream):
    return pl.pallas_call(
        forward_kernel,
        name="forward",
        out_shape=(
            jax.ShapeDtypeStruct((1024, 512), jnp.bfloat16),
            jax.ShapeDtypeStruct((16, 144, 512), jnp.bfloat16),
            jax.ShapeDtypeStruct((16, 144, 512), jnp.float32),
        ),
        in_specs=[VMEM] * 3,
        out_specs=(VMEM, VMEM, VMEM),
        scratch_shapes=[pltpu.VMEM((1152, 1536), jnp.bfloat16), pltpu.VMEM((4608, 512), jnp.float32)],
        cost_estimate=pl.CostEstimate(flops=2 * FLOPS, bytes_accessed=16 << 20, transcendentals=1 << 19),
        compiler_params=pltpu.CompilerParams(vmem_limit_bytes=40 << 20),
    )(padded_x, kernel, upstream)


def spread(padded_slope, kernel, upstream):
    return pl.pallas_call(
        spread_kernel,
        name="spread",
        out_shape=jax.ShapeDtypeStruct((1024, 512), jnp.bfloat16),
        in_specs=[VMEM] * 3,
        out_specs=VMEM,
        scratch_shapes=[pltpu.VMEM((1152, 1536), jnp.bfloat16)],
        cost_estimate=pl.CostEstimate(flops=FLOPS, bytes_accessed=8 << 20, transcendentals=0),
        compiler_params=pltpu.CompilerParams(vmem_limit_bytes=24 << 20),
    )(padded_slope, kernel, upstream)


def after(value, *gates):
    return lax.optimization_barrier((value, *gates))[0]


def exchanged(cut, axis):
    me = lax.axis_index(axis)
    sent = [cut((me + step) & 3).astype(jnp.bfloat16) for step in (1, 3, 2)]
    came = [lax.ppermute(piece, axis, ring(4, step)) for piece, step in zip(sent, (1, 3, 2))]
    total = cut(me)
    for piece in came:
        total = total + piece.astype(jnp.float32)
    return total, sent


def shards(features, upstream, kernel):
    height, breadth, channels = features.shape
    padded_x = padded(features)
    slope, goes, mine = forward(padded_x, kernel, upstream.reshape(height * breadth, channels))
    slope = slope.reshape(height, breadth, channels)

    came = lax.ppermute(goes, "core", [(0, 1), (1, 0)])
    came = came.reshape(2, 2, 4, 144, channels)
    local = mine.reshape(2, 2, 4, 144, channels)

    def cut_low(k):
        mine = lax.dynamic_slice(local, (0, 0, 0, 0, 128 * k), (2, 1, 4, 144, 128))
        other = lax.dynamic_slice(came, (0, 0, 0, 0, 128 * k), (2, 1, 4, 144, 128))
        return (mine + other.astype(jnp.float32)).reshape(2, 4, 144, 128)

    def cut_high(k):
        at = (k >> 1, 1, 0, 72 * (k & 1), 0)
        mine = lax.dynamic_slice(local, at, (1, 1, 4, 72, channels))
        other = lax.dynamic_slice(came, at, (1, 1, 4, 72, channels))
        return (mine + other.astype(jnp.float32)).reshape(4, 72, channels)

    low, sent_low = exchanged(cut_low, "x")
    high, sent_high = exchanged(cut_high, Y)

    slope = after(slope, *sent_low, *sent_high)
    padded_slope = padded(slope)

    def cut_low(k):
        piece = lax.dynamic_slice(low, (k >> 1, 0, 72 * (k & 1), 0), (1, 4, 72, 128))
        return piece.reshape(4, 72, 128)

    def cut_high(k):
        return lax.dynamic_slice(high, (0, 0, 128 * k), (4, 72, 128))

    plane_low, sent_low = exchanged(cut_low, Y)
    plane_high, sent_high = exchanged(cut_high, "x")
    plane = jnp.concatenate([plane_low, plane_high], axis=0)
    chunk = lax.all_to_all(plane, "z", 0, 0, tiled=True).sum(axis=0)
    everyone = lax.all_to_all(jnp.broadcast_to(chunk[None], (8, 72, 128)), LON, 0, 0, tiled=True)
    summed = everyone.reshape(2, 4, 72, 128).transpose(0, 2, 1, 3).reshape(144, channels)
    part = jnp.sum(everyone * everyone)
    total = lax.all_to_all(jnp.broadcast_to(part[None], (32,)), LAT, 0, 0, tiled=True).sum()

    input_grad = spread(padded_slope, kernel, upstream.reshape(height * breadth, channels))
    input_grad = input_grad.reshape(height, breadth, channels)

    count = 9.0 * channels * channels
    direction = summed / jnp.sqrt(total / count + 1e-06)
    block_rows = summed.shape[0]
    start = lax.axis_index(LAT) * block_rows
    own_kernel = lax.dynamic_slice_in_dim(kernel, start, block_rows, 0)
    perturbed = own_kernel.astype(jnp.float32) + 0.05 / jnp.sqrt(count) * direction
    return (input_grad, direction, perturbed)


def solution(mesh):
    names, sizes = zip(*SPLIT)
    fine = Mesh(mesh.devices.reshape(sizes), names)
    return jax.shard_map(
        shards,
        mesh=fine,
        in_specs=(P(LAT, LON, None), P(LAT, LON, None), P()),
        out_specs=(P(LAT, LON, None), P(LAT, None), P(LAT, None)),
        check_vma=False,
    )
```
